32 devices in a mesh: groups: 1, seq: 1, row: 16 (over z, y, core), col: 2 (over x).
Axes of the slice: x: 2, y: 2, z: 4, core: 2. Of those that a mesh axis runs over, the one named last changes fastest.
Arguments:
- paired_left: bfloat16 [512, 32, 512], P(('groups', 'seq', 'col'), None, 'row'), may hold values from -24 to 24
- paired_right: bfloat16 [512, 32, 512], P(('groups', 'seq', 'row'), None, 'col'), may hold values from -24 to 24
- unpaired_left: bfloat16 [1024, 32, 512], P(('groups', 'seq', 'col'), None, 'row'), may hold values from -24 to 24
- unpaired_right: bfloat16 [1024, 32, 512], P(('groups', 'seq', 'row'), None, 'col'), may hold values from -24 to 24
- out_weight: bfloat16 [1024, 128], replicated, may hold values from -0.1875 to 0.1875
- out_bias: float32 [128], replicated, may hold values from -6 to 6
- chain_lengths: int32 [12], P('groups'), may hold values from 1 to 128, 512 in all
- unpaired_depths: int32 [12], P('groups'), may hold values from 256 to 1024
Outputs:
- pair_update: bfloat16 [512, 512, 128], P(('groups', 'row'), ('col', 'seq'))
The draws below stay inside these ranges and needn't reach their ends.
Inputs may be any that keep to these rules, and one draw needn't show every extreme that they name: `chain_lengths`: chain lengths sum to 512. `unpaired_depths`: rows of the unpaired MSA at or beyond a chain's depth are padding.
All inputs are finite; a program needn't handle non-finite values.
Results may differ from the reference program's by a relative error of at most 0.0034.
Values may be sent and summed in bfloat16 or wider, within the bound.
A program may use at most 128 MiB of HBM per device.

```python
import math
import jax
import jax.numpy as jnp
import numpy as np
from jax import lax

C = 32
Z = 128
CHAINS = 12
S_P = 512
DMAX = 1024
N = 512
N_SEQ = 1


def place_ends(result, own_key, least, top_value):
    longest = result.shape.index(max(result.shape))
    spots = []
    for shift in (0, 1):
        where = [jax.random.randint(jax.random.fold_in(own_key, axis), (), 0, length) for axis, length in enumerate(result.shape)]
        where[longest] = (where[longest] + shift) % result.shape[longest]
        spots.append(tuple(where))
    return result.at[spots[0]].set(least).at[spots[1]].set(top_value)


def block_scale(key, shape, shards, least, high):
    level = 1.0
    for axis_at, parts in shards:
        steps = jax.random.uniform(jax.random.fold_in(jax.random.fold_in(key, 6), axis_at), (parts,), jnp.float32, least / len(shards), high / len(shards))
        level = level * jnp.repeat(jnp.exp(steps), shape[axis_at] // parts).reshape((-1,) + (1,) * (len(shape) - 1 - axis_at))
    return level


def length_profile(number_of, total, bound, skew):
    weights = [(1 << 20) // math.isqrt(rank ** skew) + 1 for rank in range(2, number_of + 1)]
    spare, given = total - bound - (number_of - 1), [1] * (number_of - 1)
    while spare > 0:
        free = [i for i in range(number_of - 1) if given[i] < bound]
        pool, left = sum([weights[i] for i in free]), spare
        for i in free:
            more = min(bound - given[i], max(1, left * weights[i] // pool), spare)
            given[i] = given[i] + more
            spare = spare - more
    return np.array([bound] + given)


def ragged_sizes(key, number_of, total, most, lean):
    if number_of == 2:
        one = jax.random.randint(key, (), max(1, total - most), min(most, total - 1) + 1)
        return jnp.stack([one, total - one])
    sizes = jnp.asarray(length_profile(number_of, total, most, lean), jnp.int32)
    couples = (number_of - 1) // 2
    source_of, taker = sizes[1:1 + 2 * couples:2], sizes[2:2 + 2 * couples:2]
    slack = jnp.minimum(source_of - 1, most - taker)
    moved = jax.random.randint(jax.random.fold_in(key, 1), (couples,), 0, 1 << 20) % (slack + 1)
    sizes = sizes.at[1:1 + 2 * couples:2].set(source_of - moved).at[2:2 + 2 * couples:2].set(taker + moved)
    return sizes[jax.random.permutation(jax.random.fold_in(key, 2), number_of)]


def scatter_about(own_key, shape, spread, bound, split=(), kind=jnp.bfloat16):
    factor_of = block_scale(own_key, shape, split, -0.22, 0.18) if split else 1.0
    values = jax.random.normal(own_key, shape, jnp.float32) * spread * factor_of
    return jnp.minimum(jnp.maximum(values, -bound), bound).astype(kind)


def setup_inputs(seed: int = 0, part: int = 0) -> dict:
    streams_of = jax.random.split(jax.random.key(seed), 9)
    part_keys = jax.random.split(jax.random.fold_in(streams_of[8], part), 9)
    paired_left = scatter_about(part_keys[0], (S_P, C, N), 4.0, 24.0, ((0, 2), (2, 16)))
    paired_right = scatter_about(part_keys[1], (S_P, C, N), 4.0, 24.0, ((0, 16), (2, 2)))
    unpaired_left = scatter_about(part_keys[2], (DMAX, C, N), 4.0, 24.0, ((0, 2), (2, 16)))
    unpaired_right = scatter_about(part_keys[3], (DMAX, C, N), 4.0, 24.0, ((0, 16), (2, 2)))
    out_weight = scatter_about(streams_of[4], (C * C, Z), (C * C) ** -0.5, 0.1875)
    out_bias = scatter_about(streams_of[5], (Z,), 1.0, 6.0, (), jnp.float32)
    chain_lengths = ragged_sizes(part_keys[6], CHAINS, N, N // 4, 1).astype(jnp.int32)
    unpaired_depths = place_ends(jax.random.randint(part_keys[7], (CHAINS,), DMAX // 4, DMAX + 1), jax.random.fold_in(part_keys[7], 1), DMAX // 4, DMAX).astype(jnp.int32)
    return {"paired_left": paired_left, "paired_right": paired_right, "unpaired_left": unpaired_left, "unpaired_right": unpaired_right, "out_weight": out_weight, "out_bias": out_bias, "chain_lengths": chain_lengths, "unpaired_depths": unpaired_depths}


def chain_tables(chain_lengths, unpaired_depths):
    positions = jnp.arange(N, dtype=jnp.int32)
    chain_ends = jnp.cumsum(chain_lengths).astype(jnp.int32)
    chain_of = jnp.sum((positions[:, None] >= chain_ends[None, :]).astype(jnp.int32), axis=1).astype(jnp.int32)
    onehot = chain_of[:, None] == jnp.arange(CHAINS, dtype=jnp.int32)[None, :]
    depth_of = jnp.sum(jnp.where(onehot, unpaired_depths[None, :], 0), axis=1).astype(jnp.int32)
    return chain_of, depth_of


def reference(paired_left, paired_right, unpaired_left, unpaired_right, out_weight, out_bias, chain_lengths, unpaired_depths):
    chain_of, depth_of = chain_tables(chain_lengths, unpaired_depths)
    free_ids = jnp.arange(DMAX, dtype=jnp.int32)
    live = (free_ids[:, None] < depth_of[None, :]).astype(unpaired_left.dtype)
    masked_left = unpaired_left * live[:, None, :]
    paired_group = S_P // N_SEQ
    free_group = DMAX // N_SEQ
    ref_rows = 8

    def one_block(block_index):
        offset = (block_index * ref_rows).astype(jnp.int32)
        chain_block = lax.dynamic_slice_in_dim(chain_of, offset, ref_rows, 0)
        depth_block = lax.dynamic_slice_in_dim(depth_of, offset, ref_rows, 0)
        same_chain = (chain_block[:, None] == chain_of[None, :]).astype(jnp.float32)
        summed = jnp.zeros((ref_rows, N, Z), jnp.float32)
        for group in range(N_SEQ):
            left_pair = lax.dynamic_slice_in_dim(paired_left[group * paired_group:(group + 1) * paired_group], offset, ref_rows, 2).astype(jnp.float32)
            right_pair = paired_right[group * paired_group:(group + 1) * paired_group].astype(jnp.float32)
            left_free = lax.dynamic_slice_in_dim(masked_left[group * free_group:(group + 1) * free_group], offset, ref_rows, 2).astype(jnp.float32)
            right_free = unpaired_right[group * free_group:(group + 1) * free_group].astype(jnp.float32)
            outer = jnp.einsum('sci,sdj->ijcd', left_pair, right_pair)
            outer = outer + jnp.einsum('sci,sdj->ijcd', left_free, right_free) * same_chain[:, :, None, None]
            outer_product = outer.astype(jnp.bfloat16).reshape(ref_rows * N, C * C)
            summed = summed + jnp.dot(outer_product, out_weight, preferred_element_type=jnp.float32).reshape(ref_rows, N, Z)
        denominator = S_P + same_chain * depth_block[:, None].astype(jnp.float32)
        return (summed / denominator[:, :, None] + out_bias).astype(jnp.bfloat16)

    blocks = lax.map(one_block, jnp.arange(N // ref_rows, dtype=jnp.int32))
    return blocks.reshape(N, N, Z)
```

```python
import functools

import jax
import jax.numpy as jnp
from jax import lax
from jax.experimental import pallas as pl
from jax.experimental.pallas import tpu as pltpu
from jax.sharding import PartitionSpec as P

LANES = 128
D_STEP = 8
WIDTH = D_STEP * LANES
LONGEST_CHAIN = 128
MESH = pl.DeviceIdType.MESH
Y_SIZE, CORES = 2, 2
AHEAD = 2
UP, DOWN, ACROSS, SIBLING = range(4)
PAIR, FREE = range(2)


def both(*terms):
    terms = [t for t in terms if t is not True]
    if any(t is False for t in terms):
        return False
    return functools.reduce(lambda a, b: a & b, terms) if terms else True


def guarded(condition, do):
    if condition is True:
        do()
    elif condition is not False:
        pl.when(condition)(do)


def fused_kernel(
    depth, width, group, paired_total, final,
    start_ref, end_ref, depth_ref,
    pair_in, free_in, left_pair_in, left_free_in, weight, bias,
    out_ref,
    pair_buf, free_buf, left_pair, left_free, outer_scr, free_scr, acc,
    send_sem, recv_sem, left_send, left_recv, local_sem,
):
    row, col = lax.axis_index("row"), lax.axis_index("col")
    core, y, z = row % CORES, (row // CORES) % Y_SIZE, row // (CORES * Y_SIZE)
    other = 1 - y
    rows, cols = out_ref.shape[0], out_ref.shape[1]
    channels = left_pair.shape[1] // rows
    tiles = cols // LANES
    steps = channels // D_STEP
    chunks = tiles * steps
    plane = rows * CORES * Y_SIZE
    span = group * channels

    def row_of(z_at, y_at, core_at):
        return (z_at * Y_SIZE + y_at) * CORES + core_at

    up, down = row_of(z + 1, y, core), row_of(z - 1, y, core)
    across, sibling = row_of(z, other, core), row_of(z, y, 1 - core)
    has_up, has_down = z < depth - 1, z > 0

    barrier = pltpu.get_barrier_semaphore()

    def greet(axis, at):
        pl.semaphore_signal(barrier, inc=1, device_id={axis: at}, device_id_type=MESH)

    pl.when(has_up)(lambda: greet("row", up))
    pl.when(has_down)(lambda: greet("row", down))
    greet("row", across)
    greet("row", sibling)
    for shift in range(1, width):
        greet("col", lax.rem(col + shift, width))
    pl.semaphore_wait(barrier, jnp.where(has_up, 1, 0) + jnp.where(has_down, 1, 0) + 2 + width - 1)

    def tile_of(chunk):
        turn = chunk // steps
        return jnp.where(col * 2 >= width, tiles - 1 - turn, turn)

    def offset(chunk):
        return pl.multiple_of((tile_of(chunk) * steps + chunk % steps) * WIDTH, WIDTH)

    def reach(kind, chunk):
        if kind == PAIR:
            return 0, depth - 1
        first = (col * tiles + tile_of(chunk)) * LANES
        lowest = jnp.maximum(first - (LONGEST_CHAIN - 1), 0) // plane
        highest = jnp.minimum(first + LANES - 1 + (LONGEST_CHAIN - 1), depth * plane - 1) // plane
        return lowest, highest

    def needed(kind, chunk):
        if kind == PAIR:
            return True
        lowest, highest = reach(kind, chunk)
        return (z >= lowest) & (z <= highest)

    def early(kind, chunk):
        return chunk % 2 == 1 if kind == PAIR else False

    sources, buffers = (pair_in, free_in), (pair_buf, free_buf)

    def copy(kind, chunk, way, origin, target, own):
        part = pl.ds(offset(chunk), WIDTH)
        here = buffers[kind].at[origin, :, part]
        return pltpu.make_async_remote_copy(
            src_ref=sources[kind].at[:, part] if own else here, dst_ref=here,
            send_sem=send_sem.at[way, kind, chunk, origin // CORES], recv_sem=recv_sem.at[kind, chunk, origin],
            device_id={"row": target}, device_id_type=MESH)

    def forward(kind, chunk, z_at, y_at, started):
        origin = row_of(z_at, y_at, core)
        line = y_at is y
        own = line and z_at is z
        lowest, highest = reach(kind, chunk)
        soon = early(kind, chunk)
        wanted = needed(kind, chunk)

        def go(way, target):
            c = copy(kind, chunk, way, origin, target, own)
            c.start() if started else c.wait_send()

        along = True if line else soon
        guarded(both(has_up, z_at <= z, z < highest, along), lambda: go(UP, up))
        guarded(both(has_down, z_at >= z, z > lowest, along), lambda: go(DOWN, down))
        if own:
            guarded(wanted, lambda: go(ACROSS, across))
        elif line:
            guarded(both(wanted, True if soon is False else jnp.logical_not(soon)), lambda: go(ACROSS, across))
        guarded(wanted, lambda: go(SIBLING, sibling))

    def arrive(kind, chunk, z_at, y_at, core_at):
        origin = row_of(z_at, y_at, core_at)
        copy(kind, chunk, SIBLING, origin, sibling, False).wait_recv()

    def hops(hop):
        if hop == 0:
            return ((z, True, True),)
        return ((z - hop, z >= hop, True), (z + hop, z + hop < depth, False))

    def arrivals(chunk, visit):
        for hop in range(depth):
            for y_at in (y, other):
                if hop == 0 and y_at is y:
                    continue
                for kind in (PAIR, FREE):
                    lowest, highest = reach(kind, chunk)
                    for z_at, there, below in hops(hop):
                        if y_at is y and kind == FREE:
                            passes = (z <= highest) if below else (z >= lowest)
                        else:
                            passes = needed(kind, chunk)
                        guarded(both(there, passes), functools.partial(visit, kind, z_at, y_at))

    def issue(chunk):
        for kind in (PAIR, FREE):
            forward(kind, chunk, z, y, True)

    def relay(chunk):
        def visit(kind, z_at, y_at):
            arrive(kind, chunk, z_at, y_at, core)
            forward(kind, chunk, z_at, y_at, True)
        arrivals(chunk, visit)

    def drain(chunk):
        for kind in (PAIR, FREE):
            forward(kind, chunk, z, y, False)
        arrivals(chunk, lambda kind, z_at, y_at: forward(kind, chunk, z_at, y_at, False))

    def gathered(chunk):
        for kind in (PAIR, FREE):
            def every(kind=kind):
                for z_at in range(depth):
                    for y_at in range(Y_SIZE):
                        arrive(kind, chunk, z_at, y_at, 1 - core)
            guarded(needed(kind, chunk), every)

    for chunk in range(min(AHEAD, chunks)):
        issue(jnp.int32(chunk))

    left_copies = []
    local = [
        pltpu.make_async_copy(pair_in, pair_buf.at[row], local_sem.at[0]),
        pltpu.make_async_copy(free_in, free_buf.at[row], local_sem.at[1]),
    ]
    for n, (source, out) in enumerate(((left_pair_in, left_pair), (left_free_in, left_free))):
        mine = out.at[col]
        for shift in range(1, width):
            c = pltpu.make_async_remote_copy(
                src_ref=source, dst_ref=mine, send_sem=left_send.at[n, shift], recv_sem=left_recv.at[n, shift],
                device_id={"col": lax.rem(col + shift, width)}, device_id_type=MESH)
            c.start()
            left_copies.append(c)
        local.append(pltpu.make_async_copy(source, mine, local_sem.at[2 + n]))
    for c in local:
        c.start()

    def left(ref, at):
        return jnp.concatenate([ref[n, at, :] for n in range(width)], axis=1)

    def compute(chunk):
        gathered(chunk)
        step = chunk % steps
        tile = tile_of(chunk)
        part = pl.ds(offset(chunk), WIDTH)
        lanes = lax.broadcasted_iota(jnp.int32, (1, LANES), 1) + tile * LANES
        mask_on = needed(FREE, chunk)

        @pl.when(step == 0)
        def _():
            acc[...] = jnp.zeros_like(acc)

        w = weight[step]

        @pl.loop(0, rows // group)
        def _(g):
            base = g * group
            at = pl.ds(pl.multiple_of(base * channels, span), span)
            right = pair_buf[:, :, part].reshape(-1, WIDTH)
            outer_scr[...] = jnp.dot(left(left_pair, at), right, preferred_element_type=jnp.float32)

            @pl.when(mask_on)
            def _():
                right = free_buf[:, :, part].reshape(-1, WIDTH)
                free_scr[...] = jnp.dot(left(left_free, at), right, preferred_element_type=jnp.float32)
                for i in range(group):
                    same = (lanes >= start_ref[base + i]) & (lanes < end_ref[base + i])
                    piece = pl.ds(i * channels, channels)
                    for d in range(D_STEP):
                        at_lanes = pl.ds(d * LANES, LANES)
                        outer_scr[piece, at_lanes] += jnp.where(same, free_scr[piece, at_lanes], 0.0)

            for pair in range(group // 2):
                halves = []
                for i in (2 * pair, 2 * pair + 1):
                    mine = outer_scr[pl.ds(i * channels, channels), :].astype(jnp.bfloat16)
                    halves.append(jnp.concatenate(
                        [mine[:, d * LANES:(d + 1) * LANES] for d in range(D_STEP)], axis=0))
                projected = jnp.dot(
                    w, jnp.concatenate(halves, axis=1), preferred_element_type=jnp.float32)
                for k in range(2):
                    acc[base + 2 * pair + k] += projected[:, k * LANES:(k + 1) * LANES]

        @pl.when(step == steps - 1)
        def _():
            @pl.loop(0, rows)
            def _(i):
                same = (lanes >= start_ref[i]) & (lanes < end_ref[i])
                count = paired_total + jnp.where(same, depth_ref[i].astype(jnp.float32), 0.0)
                value = (acc[i] * (1.0 / count)).T
                if final:
                    value = value + bias[...]
                out_ref[i, pl.ds(pl.multiple_of(tile * LANES, LANES), LANES), :] = value.astype(out_ref.dtype)

    def done_after(turn):
        return jnp.where(turn < 3, 0, jnp.minimum(turn, 2 * (turn - 2)))

    @pl.loop(0, chunks + 1)
    def _(turn):
        pl.when(turn + AHEAD < chunks)(lambda: issue(turn + AHEAD))
        pl.when(turn < chunks)(lambda: relay(turn))

        @pl.when(turn == 3)
        def _():
            for c in left_copies:
                c.wait()
            for c in local:
                c.wait()

        @pl.loop(done_after(turn - 1), done_after(turn))
        def _(chunk):
            compute(chunk)

    @pl.loop(0, chunks)
    def _(chunk):
        drain(chunk)


def fused(right_pair, right_free, left_pair, left_free, weight, bias, start, end, depth, paired_total, final):
    count, width = lax.axis_size("row"), lax.axis_size("col")
    layers = count // (Y_SIZE * CORES)
    rows = start.shape[0]
    channels = left_pair.shape[0] // rows
    out_channels = weight.shape[1]
    cols = right_pair.shape[1] // channels
    chunks = cols // LANES * (channels // D_STEP)
    group = min(16, rows)
    smem = pl.BlockSpec(memory_space=pltpu.SMEM)
    vmem = pl.BlockSpec(memory_space=pltpu.VMEM)
    anywhere = pl.BlockSpec(memory_space=pl.ANY)
    return pl.pallas_call(
        functools.partial(fused_kernel, layers, width, group, float(paired_total), final),
        out_shape=jax.ShapeDtypeStruct((rows, cols, out_channels), jnp.bfloat16 if final else jnp.float32),
        in_specs=[smem] * 3 + [anywhere] * 4 + [vmem] * 2,
        out_specs=vmem,
        scratch_shapes=[
            pltpu.VMEM((count,) + right_pair.shape, jnp.bfloat16),
            pltpu.VMEM((count,) + right_free.shape, jnp.bfloat16),
            pltpu.VMEM((width,) + left_pair.shape, jnp.bfloat16),
            pltpu.VMEM((width,) + left_free.shape, jnp.bfloat16),
            pltpu.VMEM((group * channels, WIDTH), jnp.float32),
            pltpu.VMEM((group * channels, WIDTH), jnp.float32),
            pltpu.VMEM((rows, out_channels, LANES), jnp.float32),
            pltpu.SemaphoreType.DMA((4, 2, chunks, count // CORES)),
            pltpu.SemaphoreType.DMA((2, chunks, count)),
            pltpu.SemaphoreType.DMA((2, width)),
            pltpu.SemaphoreType.DMA((2, width)),
            pltpu.SemaphoreType.DMA((4,)),
        ],
        compiler_params=pltpu.CompilerParams(collective_id=0, has_side_effects=True, vmem_limit_bytes=60 << 20),
        name="gather_multiply",
    )(start, end, depth, right_pair, right_free, left_pair, left_free, weight, bias)


def flat_right(x):
    depth, channels, cols = x.shape
    return x.reshape(depth, channels, cols // LANES, LANES).transpose(0, 2, 1, 3).reshape(depth, -1)


def flat_left(x):
    depth, channels, rows = x.shape
    return x.transpose(2, 1, 0).reshape(rows * channels, depth)


def body(
    paired_left, paired_right, unpaired_left, unpaired_right,
    out_weight, out_bias, chain_lengths, unpaired_depths,
):
    channels, rows = paired_left.shape[1:]
    cols = paired_right.shape[2]
    first_row = lax.axis_index("row") * rows
    first_col = lax.axis_index("col") * cols
    positions = first_row + jnp.arange(rows, dtype=jnp.int32)
    chains = jnp.arange(chain_lengths.shape[0])
    chain_ends = jnp.sum(
        jnp.where(chains[None, :] <= chains[:, None], chain_lengths[None, :], 0), axis=1, dtype=jnp.int32)
    chain_starts = chain_ends - chain_lengths
    inside = (positions[:, None] >= chain_starts[None, :]) & (positions[:, None] < chain_ends[None, :])

    def pick(table):
        return jnp.sum(jnp.where(inside, table[None, :], 0), axis=1, dtype=jnp.int32)

    depth = pick(unpaired_depths)
    start = pick(chain_starts) - first_col
    end = pick(chain_ends) - first_col

    seq = lax.axis_size("seq")
    free_here = unpaired_left.shape[0]
    first_free = (lax.axis_index("seq") * lax.axis_size("col") + lax.axis_index("col")) * free_here
    free_ids = first_free + jnp.arange(free_here, dtype=jnp.int32)
    live = free_ids[:, None] < depth[None, :]
    masked = jnp.where(live[:, None, :], unpaired_left, jnp.zeros((), unpaired_left.dtype))

    out_channels = out_weight.shape[1]
    weight = out_weight.reshape(channels, channels // D_STEP, D_STEP, out_channels).transpose(1, 3, 2, 0)
    weight = weight.reshape(channels // D_STEP, out_channels, D_STEP * channels)
    bias = out_bias.reshape(1, -1)
    paired_total = paired_right.shape[0] * lax.axis_size("row") * seq
    out = fused(
        flat_right(paired_right), flat_right(unpaired_right), flat_left(paired_left), flat_left(masked),
        weight, bias, start, end, depth, paired_total, seq == 1)
    if seq == 1:
        return out
    summed = lax.psum(out, "seq")
    share = cols // seq
    own = lax.dynamic_slice_in_dim(summed, lax.axis_index("seq") * share, share, 1)
    return (own + bias).astype(jnp.bfloat16)


def solution(mesh):
    return jax.shard_map(
        body,
        mesh=mesh,
        in_specs=(
            P(("groups", "seq", "col"), None, "row"),
            P(("groups", "seq", "row"), None, "col"),
            P(("groups", "seq", "col"), None, "row"),
            P(("groups", "seq", "row"), None, "col"),
            P(),
            P(),
            P("groups"),
            P("groups"),
        ),
        out_specs=P(("groups", "row"), ("col", "seq"), None),
        check_vma=False,
    )
```

```python
import functools

import jax
import jax.numpy as jnp
from jax import lax
from jax.experimental import pallas as pl
from jax.experimental.pallas import tpu as pltpu
from jax.sharding import PartitionSpec as P

LANES = 128
D_STEP = 8
WIDTH = D_STEP * LANES
LONGEST_CHAIN = 128
MESH = pl.DeviceIdType.MESH
Y_SIZE, CORES = 2, 2
AHEAD = 2
PAIR_EARLY = 4
UP, DOWN, ACROSS, SIBLING = range(4)
PAIR, FREE = range(2)


def both(*terms):
    terms = [t for t in terms if t is not True]
    if any(t is False for t in terms):
        return False
    return functools.reduce(lambda a, b: a & b, terms) if terms else True


def guarded(condition, do):
    if condition is True:
        do()
    elif condition is not False:
        pl.when(condition)(do)


def fused_kernel(
    depth, width, group, paired_total, final, share,
    start_ref, end_ref, depth_ref,
    pair_in, free_in, left_pair_in, left_free_in, weight, bias,
    out_ref,
    pair_buf, free_buf, left_pair, left_free, outer_scr, free_scr, acc, help_acc, help_out, via_buf,
    send_sem, recv_sem, left_send, left_recv, local_sem, via_send, via_recv, pass_send, help_sem,
):
    row, col = lax.axis_index("row"), lax.axis_index("col")
    core, y, z = row % CORES, (row // CORES) % Y_SIZE, row // (CORES * Y_SIZE)
    other = 1 - y
    rows, cols = out_ref.shape[0], out_ref.shape[1]
    channels = left_pair.shape[1] // rows
    tiles = cols // LANES
    steps = channels // D_STEP
    chunks = tiles * steps
    plane = rows * CORES * Y_SIZE
    span = group * channels

    def row_of(z_at, y_at, core_at):
        return (z_at * Y_SIZE + y_at) * CORES + core_at

    up, down = row_of(z + 1, y, core), row_of(z - 1, y, core)
    across, sibling = row_of(z, other, core), row_of(z, y, 1 - core)
    has_up, has_down = z < depth - 1, z > 0
    first_plane = jnp.where(col == 0, 0, depth - 1)
    last_plane = depth - 1 - first_plane
    asks = z == first_plane if share else False
    helps = z == last_plane if share else False
    distant = jnp.abs(z - last_plane) > 1 if share else False

    barrier = pltpu.get_barrier_semaphore()

    def greet(axis, at):
        pl.semaphore_signal(barrier, inc=1, device_id={axis: at}, device_id_type=MESH)

    pl.when(has_up)(lambda: greet("row", up))
    pl.when(has_down)(lambda: greet("row", down))
    greet("row", across)
    greet("row", sibling)
    for shift in range(1, width):
        greet("col", lax.rem(col + shift, width))
    met = jnp.where(has_up, 1, 0) + jnp.where(has_down, 1, 0) + 2 + width - 1
    if share:
        for hop in range(2, depth):
            far = jnp.where(last_plane == 0, hop, depth - 1 - hop)
            pl.when(helps)(functools.partial(greet, "row", row_of(far, y, core)))
        met = met + jnp.where(distant, 1, 0)
    pl.semaphore_wait(barrier, met)

    def tile_of(chunk, at_col=col):
        turn = chunk % tiles
        return jnp.where(at_col * 2 >= width, turn, tiles - 1 - turn)

    def offset(chunk, at_col=col):
        return pl.multiple_of((tile_of(chunk, at_col) * steps + chunk // tiles) * WIDTH, WIDTH)

    def reach(kind, chunk):
        if kind == PAIR:
            return 0, depth - 1
        first = (col * tiles + tile_of(chunk)) * LANES
        lowest = jnp.maximum(first - (LONGEST_CHAIN - 1), 0) // plane
        highest = jnp.minimum(first + LANES - 1 + (LONGEST_CHAIN - 1), depth * plane - 1) // plane
        if share:
            shared = chunk % tiles == 0
            lowest = jnp.where(shared & (col == 0), jnp.maximum(lowest, 1), lowest)
            highest = jnp.where(shared & (col > 0), jnp.minimum(highest, depth - 2), highest)
        return lowest, highest

    def needed(kind, chunk):
        if kind == PAIR:
            return True
        lowest, highest = reach(kind, chunk)
        return (z >= lowest) & (z <= highest)

    def early(kind, chunk):
        if kind == PAIR:
            return chunk % PAIR_EARLY == 0
        return chunk % tiles == 0 if share else False

    def late(kind, chunk):
        soon = early(kind, chunk)
        return True if soon is False else jnp.logical_not(soon)

    sources, buffers = (pair_in, free_in), (pair_buf, free_buf)

    def copy(kind, chunk, way, origin, target, own):
        part = pl.ds(offset(chunk), WIDTH)
        here = buffers[kind].at[origin, :, part]
        return pltpu.make_async_remote_copy(
            src_ref=sources[kind].at[:, part] if own else here, dst_ref=here,
            send_sem=send_sem.at[way, kind, chunk, origin // CORES], recv_sem=recv_sem.at[kind, chunk, origin],
            device_id={"row": target}, device_id_type=MESH)

    def move(c, started):
        c.start() if started else c.wait_send()

    def forward(kind, chunk, z_at, y_at, started):
        origin = row_of(z_at, y_at, core)
        line = y_at is y
        own = line and z_at is z
        lowest, highest = reach(kind, chunk)
        soon = early(kind, chunk)
        wanted = needed(kind, chunk)

        def go(way, target):
            move(copy(kind, chunk, way, origin, target, own), started)

        along = True if line else soon
        guarded(both(has_up, z_at <= z, z < highest, along), lambda: go(UP, up))
        guarded(both(has_down, z_at >= z, z > lowest, along), lambda: go(DOWN, down))
        if own:
            guarded(wanted if wanted is True or soon is False else wanted | soon, lambda: go(ACROSS, across))
        elif line:
            guarded(both(wanted, late(kind, chunk)), lambda: go(ACROSS, across))
        guarded(wanted, lambda: go(SIBLING, sibling))

    def arrive(kind, chunk, z_at, y_at, core_at):
        origin = row_of(z_at, y_at, core_at)
        copy(kind, chunk, SIBLING, origin, sibling, False).wait_recv()

    def hops(hop):
        if hop == 0:
            return ((z, True, None),)
        return ((z - hop, z >= hop, True), (z + hop, z + hop < depth, False))

    def arrivals(hop, y_at, chunk, visit):
        for kind in (PAIR, FREE):
            lowest, highest = reach(kind, chunk)
            for z_at, there, below in hops(hop):
                passes = True
                if kind == FREE and below is not None:
                    passes = (z <= highest) if below else (z >= lowest)
                if y_at is not y and kind == FREE:
                    soon = early(kind, chunk)
                    if soon is False:
                        passes = needed(kind, chunk)
                    else:
                        passes = (soon & passes) | (jnp.logical_not(soon) & needed(kind, chunk))
                guarded(both(there, passes), functools.partial(visit, kind, z_at, y_at))

    def onward(chunk, started):
        def visit(kind, z_at, y_at):
            if started:
                arrive(kind, chunk, z_at, y_at, core)
            forward(kind, chunk, z_at, y_at, started)
        return visit

    def slot(part):
        return part * tiles + 1

    def helping(turn, do):
        part = turn - turn // 3
        pl.when((turn >= 0) & (turn % 3 < 2) & (part < steps))(lambda: do(part))

    def via_copy(part, straight):
        target = free_buf.at[row, :, pl.ds(offset(slot(part), 1 - col), WIDTH)] if straight else via_buf.at[part]
        return pltpu.make_async_remote_copy(
            src_ref=free_in.at[:, pl.ds(offset(part * tiles), WIDTH)], dst_ref=target,
            send_sem=via_send.at[part], recv_sem=via_recv.at[part], device_id={"col": 1 - col}, device_id_type=MESH)

    def pass_copy(part):
        return pltpu.make_async_remote_copy(
            src_ref=via_buf.at[part], dst_ref=free_buf.at[row, :, pl.ds(offset(slot(part)), WIDTH)],
            send_sem=pass_send.at[part], recv_sem=recv_sem.at[FREE, slot(part), row],
            device_id={"row": row_of(last_plane, y, core)}, device_id_type=MESH)

    def via(part, started):
        pl.when(asks)(lambda: move(via_copy(part, True), started))
        pl.when(jnp.logical_not(asks))(lambda: move(via_copy(part, False), started))

    def help_spread(part, z_at, y_at, started):
        origin = row_of(z_at, y_at, core)
        if y_at is y:
            move(copy(FREE, slot(part), ACROSS, origin, across, False), started)
        move(copy(FREE, slot(part), SIBLING, origin, sibling, False), started)

    def help_first(part, started):
        if started:
            via_copy(part, False).wait_recv()

        @pl.when(jnp.logical_not(helps))
        def _():
            move(pass_copy(part), started)

        @pl.when(helps)
        def _():
            help_spread(part, z, y, started)

    def help_line(part, started):
        @pl.when(helps)
        def _():
            for hop in range(1, depth):
                z_at = jnp.where(last_plane == 0, hop, depth - 1 - hop)
                if started:
                    arrive(FREE, slot(part), z_at, y, core)
                help_spread(part, z_at, y, started)

    def help_last(part, started):
        @pl.when(helps)
        def _():
            for hop in range(depth):
                z_at = jnp.where(last_plane == 0, hop, depth - 1 - hop)
                if started:
                    arrive(FREE, slot(part), z_at, other, core)
                help_spread(part, z_at, other, started)

    def result_copy():
        return pltpu.make_async_remote_copy(
            src_ref=help_out, dst_ref=help_out, send_sem=help_sem.at[0], recv_sem=help_sem.at[1],
            device_id={"col": 1 - col}, device_id_type=MESH)

    def issue(chunk, started=True):
        for kind in (PAIR, FREE):
            forward(kind, chunk, z, y, started)

    def within(chunk, limit, do):
        pl.when((chunk >= 0) & (chunk < limit))(lambda: do(chunk))

    def relay(turn):
        for hop in range(depth - 1, 0, -1):
            within(turn - (hop - 1), chunks, lambda chunk: arrivals(hop, y, chunk, onward(chunk, True)))
        if share:
            helping(turn, lambda part: help_first(part, True))
            helping(turn - 1, lambda part: help_line(part, True))
        for hop in range(depth - 1, -1, -1):
            within(turn - hop, chunks, lambda chunk: arrivals(hop, other, chunk, onward(chunk, True)))
        if share:
            helping(turn - 2, lambda part: help_last(part, True))
            helping(turn + AHEAD, lambda part: via(part, True))
        within(turn + AHEAD, chunks, issue)

    def drain(chunk):
        issue(chunk, False)
        for hop in range(depth):
            if hop:
                arrivals(hop, y, chunk, onward(chunk, False))
            arrivals(hop, other, chunk, onward(chunk, False))
        if share:
            @pl.when(chunk < steps)
            def _():
                via(chunk, False)
                help_first(chunk, False)
                help_line(chunk, False)
                help_last(chunk, False)

    def from_sibling(kind, chunk):
        for z_at in range(depth):
            for y_at in range(Y_SIZE):
                arrive(kind, chunk, z_at, y_at, 1 - core)

    def gathered(chunk):
        for kind in (PAIR, FREE):
            guarded(needed(kind, chunk), functools.partial(from_sibling, kind, chunk))

    for chunk in range(min(AHEAD, chunks)):
        if share:
            helping(jnp.int32(chunk), lambda part: via(part, True))
        issue(jnp.int32(chunk))

    left_copies = []
    local = [pltpu.make_async_copy(pair_in, pair_buf.at[row], local_sem.at[0])]
    own_free = pltpu.make_async_copy(free_in, free_buf.at[row], local_sem.at[1])
    unhelping = jnp.logical_not(helps) if share else True
    for n, (source, out) in enumerate(((left_pair_in, left_pair), (left_free_in, left_free))):
        mine = out.at[col]
        for shift in range(1, width):
            c = pltpu.make_async_remote_copy(
                src_ref=source, dst_ref=mine, send_sem=left_send.at[n, shift], recv_sem=left_recv.at[n, shift],
                device_id={"col": lax.rem(col + shift, width)}, device_id_type=MESH)
            c.start()
            left_copies.append(c)
        local.append(pltpu.make_async_copy(source, mine, local_sem.at[2 + n]))
    for c in local:
        c.start()
    guarded(unhelping, own_free.start)

    def left(ref, at):
        return jnp.concatenate([ref[n, at, :] for n in range(width)], axis=1)

    def same_at(first, i):
        lanes = lax.broadcasted_iota(jnp.int32, (1, LANES), 1) + first * LANES
        return (lanes >= start_ref[i]) & (lanes < end_ref[i])

    def project(w, scratch, total, base):
        for pair in range(group // 2):
            halves = []
            for i in (2 * pair, 2 * pair + 1):
                mine = scratch[pl.ds(i * channels, channels), :].astype(jnp.bfloat16)
                halves.append(jnp.concatenate(
                    [mine[:, d * LANES:(d + 1) * LANES] for d in range(D_STEP)], axis=0))
            projected = jnp.dot(w, jnp.concatenate(halves, axis=1), preferred_element_type=jnp.float32)
            for k in range(2):
                total[base + 2 * pair + k] += projected[:, k * LANES:(k + 1) * LANES]

    def compute(chunk):
        if tiles > 1:
            @pl.when(chunk == chunks - 1)
            def _():
                for done in range(tiles - 1):
                    finish(done)

        gathered(chunk)
        step = chunk // tiles
        turn = chunk % tiles
        first = col * tiles + tile_of(chunk)
        part = pl.ds(offset(chunk), WIDTH)
        mask_on = needed(FREE, chunk)
        total = acc.at[turn]
        w = weight[step]

        @pl.when(step == 0)
        def _():
            total[...] = jnp.zeros_like(total)

        @pl.loop(0, rows // group)
        def _(g):
            base = g * group
            at = pl.ds(pl.multiple_of(base * channels, span), span)
            right = pair_buf[:, :, part].reshape(-1, WIDTH)
            outer_scr[...] = jnp.dot(left(left_pair, at), right, preferred_element_type=jnp.float32)

            @pl.when(mask_on)
            def _():
                right = free_buf[:, :, part].reshape(-1, WIDTH)
                free_scr[...] = jnp.dot(left(left_free, at), right, preferred_element_type=jnp.float32)
                for i in range(group):
                    same = same_at(first, base + i)
                    piece = pl.ds(i * channels, channels)
                    for d in range(D_STEP):
                        at_lanes = pl.ds(d * LANES, LANES)
                        outer_scr[piece, at_lanes] += jnp.where(same, free_scr[piece, at_lanes], 0.0)

            project(w, outer_scr, total, base)

        pl.when(chunk == chunks - 1)(lambda: finish(tiles - 1))

    def help_compute(q):
        from_sibling(FREE, slot(q))
        w = weight[q]
        first = (1 - col) * tiles + tile_of(q * tiles, 1 - col)
        part = pl.ds(offset(slot(q)), WIDTH)

        @pl.when(q == 0)
        def _():
            help_acc[...] = jnp.zeros_like(help_acc)

        @pl.loop(0, rows // group)
        def _(g):
            base = g * group
            at = pl.ds(pl.multiple_of(base * channels, span), span)
            right = free_buf[:, :, part].reshape(-1, WIDTH)
            free_scr[...] = jnp.dot(left(left_free, at), right, preferred_element_type=jnp.float32)
            for i in range(group):
                same = same_at(first, base + i)
                piece = pl.ds(i * channels, channels)
                for d in range(D_STEP):
                    at_lanes = pl.ds(d * LANES, LANES)
                    free_scr[piece, at_lanes] = jnp.where(same, free_scr[piece, at_lanes], 0.0)
            project(w, free_scr, help_acc, base)

        @pl.when(q == steps - 1)
        def _():
            @pl.loop(0, rows)
            def _(i):
                count = paired_total + depth_ref[i].astype(jnp.float32)
                help_out[i] = (help_acc[i] * (1.0 / count)).T.astype(help_out.dtype)

            result_copy().start()

    def write(turn, helped):
        tile = tile_of(turn)

        @pl.loop(0, rows)
        def _(i):
            same = same_at(col * tiles + tile, i)
            count = paired_total + jnp.where(same, depth_ref[i].astype(jnp.float32), 0.0)
            value = (acc[turn, i] * (1.0 / count)).T
            if helped:
                value = value + help_out[i].astype(jnp.float32)
            if final:
                value = value + bias[...]
            out_ref[i, pl.ds(pl.multiple_of(tile * LANES, LANES), LANES), :] = value.astype(out_ref.dtype)

    def finish(turn):
        if share and turn == 0:
            @pl.when(asks)
            def _():
                result_copy().wait_recv()
                write(turn, True)

            pl.when(jnp.logical_not(asks))(functools.partial(write, turn, False))
        else:
            write(turn, False)

    def done_after(turn):
        return jnp.clip(turn - depth + 1, 0, chunks)

    @pl.loop(0, chunks + depth)
    def _(turn):
        relay(turn)

        @pl.when(turn == depth)
        def _():
            for c in left_copies:
                c.wait()
            for c in local:
                c.wait()
            guarded(unhelping, own_free.wait)

        if share:
            helping(turn - depth, lambda q: pl.when(helps)(lambda: help_compute(q)))

        @pl.loop(done_after(turn - 1), done_after(turn))
        def _(chunk):
            compute(chunk)

    @pl.loop(0, chunks)
    def _(chunk):
        drain(chunk)

    if share:
        pl.when(helps)(lambda: result_copy().wait_send())


def fused(right_pair, right_free, left_pair, left_free, weight, bias, start, end, depth, paired_total, final):
    count, width = lax.axis_size("row"), lax.axis_size("col")
    layers = count // (Y_SIZE * CORES)
    rows = start.shape[0]
    channels = left_pair.shape[0] // rows
    out_channels = weight.shape[1]
    cols = right_pair.shape[1] // channels
    tiles, steps = cols // LANES, channels // D_STEP
    chunks = tiles * steps
    group = min(16, rows)
    share = width == 2 and tiles == 2 and layers == width * tiles and rows * count == layers * LANES
    smem = pl.BlockSpec(memory_space=pltpu.SMEM)
    vmem = pl.BlockSpec(memory_space=pltpu.VMEM)
    anywhere = pl.BlockSpec(memory_space=pl.ANY)
    helped = (rows, out_channels, LANES) if share else (8, 8, LANES)
    return pl.pallas_call(
        functools.partial(fused_kernel, layers, width, group, float(paired_total), final, share),
        out_shape=jax.ShapeDtypeStruct((rows, cols, out_channels), jnp.bfloat16 if final else jnp.float32),
        in_specs=[smem] * 3 + [anywhere] * 4 + [vmem] * 2,
        out_specs=vmem,
        scratch_shapes=[
            pltpu.VMEM((count,) + right_pair.shape, jnp.bfloat16),
            pltpu.VMEM((count,) + right_free.shape, jnp.bfloat16),
            pltpu.VMEM((width,) + left_pair.shape, jnp.bfloat16),
            pltpu.VMEM((width,) + left_free.shape, jnp.bfloat16),
            pltpu.VMEM((group * channels, WIDTH), jnp.float32),
            pltpu.VMEM((group * channels, WIDTH), jnp.float32),
            pltpu.VMEM((tiles, rows, out_channels, LANES), jnp.float32),
            pltpu.VMEM(helped, jnp.float32),
            pltpu.VMEM((helped[0], helped[2], helped[1]), jnp.bfloat16),
            pltpu.VMEM((steps if share else 1, right_free.shape[0], WIDTH), jnp.bfloat16),
            pltpu.SemaphoreType.DMA((4, 2, chunks, count // CORES)),
            pltpu.SemaphoreType.DMA((2, chunks, count)),
            pltpu.SemaphoreType.DMA((2, width)),
            pltpu.SemaphoreType.DMA((2, width)),
            pltpu.SemaphoreType.DMA((4,)),
            pltpu.SemaphoreType.DMA((steps,)),
            pltpu.SemaphoreType.DMA((steps,)),
            pltpu.SemaphoreType.DMA((steps,)),
            pltpu.SemaphoreType.DMA((2,)),
        ],
        compiler_params=pltpu.CompilerParams(collective_id=0, has_side_effects=True, vmem_limit_bytes=60 << 20),
        name="gather_multiply",
    )(start, end, depth, right_pair, right_free, left_pair, left_free, weight, bias)


def flat_right(x):
    depth, channels, cols = x.shape
    return x.reshape(depth, channels, cols // LANES, LANES).transpose(0, 2, 1, 3).reshape(depth, -1)


def flat_left(x):
    depth, channels, rows = x.shape
    return x.transpose(2, 1, 0).reshape(rows * channels, depth)


def body(
    paired_left, paired_right, unpaired_left, unpaired_right,
    out_weight, out_bias, chain_lengths, unpaired_depths,
):
    channels, rows = paired_left.shape[1:]
    cols = paired_right.shape[2]
    first_row = lax.axis_index("row") * rows
    positions = first_row + jnp.arange(rows, dtype=jnp.int32)
    chains = jnp.arange(chain_lengths.shape[0])
    chain_ends = jnp.sum(
        jnp.where(chains[None, :] <= chains[:, None], chain_lengths[None, :], 0), axis=1, dtype=jnp.int32)
    chain_starts = chain_ends - chain_lengths
    inside = (positions[:, None] >= chain_starts[None, :]) & (positions[:, None] < chain_ends[None, :])

    def pick(table):
        return jnp.sum(jnp.where(inside, table[None, :], 0), axis=1, dtype=jnp.int32)

    depth = pick(unpaired_depths)
    start = pick(chain_starts)
    end = pick(chain_ends)

    seq = lax.axis_size("seq")
    free_here = unpaired_left.shape[0]
    first_free = (lax.axis_index("seq") * lax.axis_size("col") + lax.axis_index("col")) * free_here
    free_ids = first_free + jnp.arange(free_here, dtype=jnp.int32)
    live = free_ids[:, None] < depth[None, :]
    masked = jnp.where(live[:, None, :], unpaired_left, jnp.zeros((), unpaired_left.dtype))

    out_channels = out_weight.shape[1]
    weight = out_weight.reshape(channels, channels // D_STEP, D_STEP, out_channels).transpose(1, 3, 2, 0)
    weight = weight.reshape(channels // D_STEP, out_channels, D_STEP * channels)
    bias = out_bias.reshape(1, -1)
    paired_total = paired_right.shape[0] * lax.axis_size("row") * seq
    out = fused(
        flat_right(paired_right), flat_right(unpaired_right), flat_left(paired_left), flat_left(masked),
        weight, bias, start, end, depth, paired_total, seq == 1)
    if seq == 1:
        return out
    summed = lax.psum(out, "seq")
    share = cols // seq
    own = lax.dynamic_slice_in_dim(summed, lax.axis_index("seq") * share, share, 1)
    return (own + bias).astype(jnp.bfloat16)


def solution(mesh):
    return jax.shard_map(
        body,
        mesh=mesh,
        in_specs=(
            P(("groups", "seq", "col"), None, "row"),
            P(("groups", "seq", "row"), None, "col"),
            P(("groups", "seq", "col"), None, "row"),
            P(("groups", "seq", "row"), None, "col"),
            P(),
            P(),
            P("groups"),
            P("groups"),
        ),
        out_specs=P(("groups", "row"), ("col", "seq"), None),
        check_vma=False,
    )
```

```python
import functools

import jax
import jax.numpy as jnp
from jax import lax
from jax.experimental import pallas as pl
from jax.experimental.pallas import tpu as pltpu
from jax.sharding import PartitionSpec as P

LANES = 128
D_STEP = 8
WIDTH = D_STEP * LANES
LONGEST_CHAIN = 128
MESH = pl.DeviceIdType.MESH
Y_SIZE, CORES = 2, 2
AHEAD = 2
HELP_LAG = 3
PAIR_EARLY = 4
UP, DOWN, ACROSS, SIBLING = range(4)
PAIR, FREE = range(2)


def both(*terms):
    terms = [t for t in terms if t is not True]
    if any(t is False for t in terms):
        return False
    return functools.reduce(lambda a, b: a & b, terms) if terms else True


def guarded(condition, do):
    if condition is True:
        do()
    elif condition is not False:
        pl.when(condition)(do)


def fused_kernel(
    depth, width, group, paired_total, final, share,
    lengths_ref, depths_ref,
    pair_in, free_in, left_pair_in, left_free_in, plain_weight, bias,
    out_ref,
    start_ref, end_ref, depth_ref, weight, wide_weight, spread, raw_pair, raw_free,
    pair_buf, free_buf, left_pair, left_free, outer_scr, free_scr, acc, help_acc, help_out, via_buf,
    send_sem, recv_sem, left_send, left_recv, local_sem, via_send, via_recv, pass_send, help_sem,
):
    row, col = lax.axis_index("row"), lax.axis_index("col")
    core, y, z = row % CORES, (row // CORES) % Y_SIZE, row // (CORES * Y_SIZE)
    other = 1 - y
    rows, cols = out_ref.shape[0], out_ref.shape[1]
    channels = left_pair.shape[1] // rows
    tiles = cols // LANES
    steps = channels // D_STEP
    chunks = tiles * steps
    plane = rows * CORES * Y_SIZE
    span = group * channels

    def row_of(z_at, y_at, core_at):
        return (z_at * Y_SIZE + y_at) * CORES + core_at

    up, down = row_of(z + 1, y, core), row_of(z - 1, y, core)
    across, sibling = row_of(z, other, core), row_of(z, y, 1 - core)
    has_up, has_down = z < depth - 1, z > 0
    first_plane = jnp.where(col == 0, 0, depth - 1)
    last_plane = depth - 1 - first_plane
    asks = z == first_plane if share else False
    helps = z == last_plane if share else False
    distant = jnp.abs(z - last_plane) > 1 if share else False

    barrier = pltpu.get_barrier_semaphore()

    def greet(axis, at):
        pl.semaphore_signal(barrier, inc=1, device_id={axis: at}, device_id_type=MESH)

    pl.when(has_up)(lambda: greet("row", up))
    pl.when(has_down)(lambda: greet("row", down))
    greet("row", across)
    greet("row", sibling)
    for shift in range(1, width):
        greet("col", lax.rem(col + shift, width))
    met = jnp.where(has_up, 1, 0) + jnp.where(has_down, 1, 0) + 2 + width - 1
    if share:
        for hop in range(2, depth):
            far = jnp.where(last_plane == 0, hop, depth - 1 - hop)
            pl.when(helps)(functools.partial(greet, "row", row_of(far, y, core)))
        met = met + jnp.where(distant, 1, 0)
    pl.semaphore_wait(barrier, met)

    def tile_of(chunk, at_col=col):
        turn = chunk % tiles
        return jnp.where(at_col * 2 >= width, turn, tiles - 1 - turn)

    def offset(chunk, at_col=col):
        return pl.multiple_of((tile_of(chunk, at_col) * steps + chunk // tiles) * WIDTH, WIDTH)

    def reach(kind, chunk):
        if kind == PAIR:
            return 0, depth - 1
        first = (col * tiles + tile_of(chunk)) * LANES
        lowest = jnp.maximum(first - (LONGEST_CHAIN - 1), 0) // plane
        highest = jnp.minimum(first + LANES - 1 + (LONGEST_CHAIN - 1), depth * plane - 1) // plane
        if share:
            shared = chunk % tiles == 0
            lowest = jnp.where(shared & (col == 0), jnp.maximum(lowest, 1), lowest)
            highest = jnp.where(shared & (col > 0), jnp.minimum(highest, depth - 2), highest)
        return lowest, highest

    def needed(kind, chunk):
        if kind == PAIR:
            return True
        lowest, highest = reach(kind, chunk)
        return (z >= lowest) & (z <= highest)

    def early(kind, chunk):
        if kind == PAIR:
            return chunk % PAIR_EARLY == 0
        return chunk % tiles == 0 if share else False

    def late(kind, chunk):
        soon = early(kind, chunk)
        return True if soon is False else jnp.logical_not(soon)

    sources, buffers = (pair_in, free_in), (pair_buf, free_buf)

    def copy(kind, chunk, way, origin, target, own):
        part = pl.ds(offset(chunk), WIDTH)
        here = buffers[kind].at[origin, :, part]
        return pltpu.make_async_remote_copy(
            src_ref=sources[kind].at[:, part] if own else here, dst_ref=here,
            send_sem=send_sem.at[way, kind, chunk, origin // CORES], recv_sem=recv_sem.at[kind, chunk, origin],
            device_id={"row": target}, device_id_type=MESH)

    def move(c, started):
        c.start() if started else c.wait_send()

    def forward(kind, chunk, z_at, y_at, started):
        origin = row_of(z_at, y_at, core)
        line = y_at is y
        own = line and z_at is z
        lowest, highest = reach(kind, chunk)
        soon = early(kind, chunk)
        wanted = needed(kind, chunk)

        def go(way, target):
            move(copy(kind, chunk, way, origin, target, own), started)

        along = True if line else soon
        guarded(both(has_up, z_at <= z, z < highest, along), lambda: go(UP, up))
        guarded(both(has_down, z_at >= z, z > lowest, along), lambda: go(DOWN, down))
        if own:
            guarded(wanted if wanted is True or soon is False else wanted | soon, lambda: go(ACROSS, across))
        elif line:
            guarded(both(wanted, late(kind, chunk)), lambda: go(ACROSS, across))
        guarded(wanted, lambda: go(SIBLING, sibling))

    def arrive(kind, chunk, z_at, y_at, core_at):
        origin = row_of(z_at, y_at, core_at)
        copy(kind, chunk, SIBLING, origin, sibling, False).wait_recv()

    def hops(hop):
        if hop == 0:
            return ((z, True, None),)
        return ((z - hop, z >= hop, True), (z + hop, z + hop < depth, False))

    def arrivals(hop, y_at, chunk, visit):
        for kind in (PAIR, FREE):
            lowest, highest = reach(kind, chunk)
            for z_at, there, below in hops(hop):
                passes = True
                if kind == FREE and below is not None:
                    passes = (z <= highest) if below else (z >= lowest)
                if y_at is not y and kind == FREE:
                    soon = early(kind, chunk)
                    if soon is False:
                        passes = needed(kind, chunk)
                    else:
                        passes = (soon & passes) | (jnp.logical_not(soon) & needed(kind, chunk))
                guarded(both(there, passes), functools.partial(visit, kind, z_at, y_at))

    def onward(chunk, started):
        def visit(kind, z_at, y_at):
            if started:
                arrive(kind, chunk, z_at, y_at, core)
            forward(kind, chunk, z_at, y_at, started)
        return visit

    def slot(part):
        return part * tiles + 1

    def helping(turn, do):
        part = turn - turn // 3
        pl.when((turn >= 0) & (turn % 3 < 2) & (part < steps))(lambda: do(part))

    def via_copy(part, straight):
        target = free_buf.at[row, :, pl.ds(offset(slot(part), 1 - col), WIDTH)] if straight else via_buf.at[part]
        return pltpu.make_async_remote_copy(
            src_ref=free_in.at[:, pl.ds(offset(part * tiles), WIDTH)], dst_ref=target,
            send_sem=via_send.at[part], recv_sem=via_recv.at[part], device_id={"col": 1 - col}, device_id_type=MESH)

    def pass_copy(part):
        return pltpu.make_async_remote_copy(
            src_ref=via_buf.at[part], dst_ref=free_buf.at[row, :, pl.ds(offset(slot(part)), WIDTH)],
            send_sem=pass_send.at[part], recv_sem=recv_sem.at[FREE, slot(part), row],
            device_id={"row": row_of(last_plane, y, core)}, device_id_type=MESH)

    def via(part, started):
        pl.when(asks)(lambda: move(via_copy(part, True), started))
        pl.when(jnp.logical_not(asks))(lambda: move(via_copy(part, False), started))

    def help_spread(part, z_at, y_at, started):
        origin = row_of(z_at, y_at, core)
        if y_at is y:
            move(copy(FREE, slot(part), ACROSS, origin, across, False), started)
        move(copy(FREE, slot(part), SIBLING, origin, sibling, False), started)

    def help_first(part, started):
        if started:
            via_copy(part, False).wait_recv()

        @pl.when(jnp.logical_not(helps))
        def _():
            move(pass_copy(part), started)

        @pl.when(helps)
        def _():
            help_spread(part, z, y, started)

    def help_line(part, started):
        @pl.when(helps)
        def _():
            for hop in range(1, depth):
                z_at = jnp.where(last_plane == 0, hop, depth - 1 - hop)
                if started:
                    arrive(FREE, slot(part), z_at, y, core)
                help_spread(part, z_at, y, started)

    def help_last(part, started):
        @pl.when(helps)
        def _():
            for hop in range(depth):
                z_at = jnp.where(last_plane == 0, hop, depth - 1 - hop)
                if started:
                    arrive(FREE, slot(part), z_at, other, core)
                help_spread(part, z_at, other, started)

    def result_copy():
        return pltpu.make_async_remote_copy(
            src_ref=help_out, dst_ref=help_out, send_sem=help_sem.at[0], recv_sem=help_sem.at[1],
            device_id={"col": 1 - col}, device_id_type=MESH)

    def issue(chunk, started=True):
        for kind in (PAIR, FREE):
            forward(kind, chunk, z, y, started)

    def within(chunk, limit, do):
        pl.when((chunk >= 0) & (chunk < limit))(lambda: do(chunk))

    def relay_line(turn):
        for hop in range(depth - 1, 0, -1):
            within(turn - (hop - 1), chunks, lambda chunk: arrivals(hop, y, chunk, onward(chunk, True)))
        if share:
            helping(turn, lambda part: help_first(part, True))
            helping(turn - 1, lambda part: help_line(part, True))

    def relay_across(turn):
        for hop in range(depth - 1, -1, -1):
            within(turn - hop, chunks, lambda chunk: arrivals(hop, other, chunk, onward(chunk, True)))
        if share:
            helping(turn - 2, lambda part: help_last(part, True))
            helping(turn + AHEAD, lambda part: via(part, True))
        within(turn + AHEAD, chunks, issue)

    def drain(chunk):
        issue(chunk, False)
        for hop in range(depth):
            if hop:
                arrivals(hop, y, chunk, onward(chunk, False))
            arrivals(hop, other, chunk, onward(chunk, False))
        if share:
            @pl.when(chunk < steps)
            def _():
                via(chunk, False)
                help_first(chunk, False)
                help_line(chunk, False)
                help_last(chunk, False)

    def from_sibling(kind, chunk):
        for z_at in range(depth):
            for y_at in range(Y_SIZE):
                arrive(kind, chunk, z_at, y_at, 1 - core)

    def gathered(chunk):
        for kind in (PAIR, FREE):
            guarded(needed(kind, chunk), functools.partial(from_sibling, kind, chunk))

    for chunk in range(min(AHEAD, chunks)):
        if share:
            helping(jnp.int32(chunk), lambda part: via(part, True))
        issue(jnp.int32(chunk))

    left_copies = []
    local = [pltpu.make_async_copy(pair_in, pair_buf.at[row], local_sem.at[0])]
    own_free = pltpu.make_async_copy(free_in, free_buf.at[row], local_sem.at[1])
    unhelping = jnp.logical_not(helps) if share else True
    for n, (source, out) in enumerate(((left_pair_in, raw_pair), (left_free_in, raw_free))):
        mine = out.at[col]
        for shift in range(1, width):
            c = pltpu.make_async_remote_copy(
                src_ref=source, dst_ref=mine, send_sem=left_send.at[n, shift], recv_sem=left_recv.at[n, shift],
                device_id={"col": lax.rem(col + shift, width)}, device_id_type=MESH)
            c.start()
            left_copies.append(c)
        local.append(pltpu.make_async_copy(source, mine, local_sem.at[2 + n]))
    for c in local:
        c.start()
    guarded(unhelping, own_free.start)

    @pl.loop(0, rows)
    def _(i):
        place = row * rows + i
        end, start, stop, deep = jnp.int32(0), jnp.int32(0), jnp.int32(0), jnp.int32(0)
        for k in range(lengths_ref.shape[0]):
            begin, end = end, end + lengths_ref[k]
            mine = (place >= begin) & (place < end)
            start = jnp.where(mine, begin, start)
            stop = jnp.where(mine, end, stop)
            deep = jnp.where(mine, depths_ref[k], deep)
        start_ref[i], end_ref[i], depth_ref[i] = start, stop, deep

    wide_weight[...] = plain_weight[...].astype(jnp.float32)
    for step in range(steps):
        picked = [wide_weight[pl.ds(step * D_STEP + d, channels, stride=channels), :] for d in range(D_STEP)]
        weight[step] = jnp.concatenate(picked, axis=0).T.astype(jnp.bfloat16)

    def arrange(raw, arranged, masked):
        length = raw.shape[2]
        wide = min(length, LANES)
        for n in range(width):
            for low in range(0, length, wide):
                ids = lax.broadcasted_iota(jnp.int32, (1, LANES), 1) + n * length + low
                if masked:
                    ids = ids + lax.axis_index("seq") * (width * length)
                spread[:, :wide] = raw[n, :, low:low + wide].astype(jnp.float32)

                @pl.loop(0, rows, unroll=4)
                def _(i):
                    value = spread[pl.ds(i, channels, stride=rows), :]
                    if masked:
                        value = jnp.where(ids < depth_ref[i], value, 0.0)
                    at = pl.ds(pl.multiple_of(i * channels, channels), channels)
                    arranged[n, at, low:low + wide] = value[:, :wide].astype(jnp.bfloat16)

    def left(ref, at):
        return jnp.concatenate([ref[n, at, :] for n in range(width)], axis=1)

    def same_at(first, i):
        lanes = lax.broadcasted_iota(jnp.int32, (1, LANES), 1) + first * LANES
        return (lanes >= start_ref[i]) & (lanes < end_ref[i])

    def project(w, load, total, base):
        for pair in range(group // 2):
            halves = []
            for i in (2 * pair, 2 * pair + 1):
                same = same_at(load.first, base + i) if load.masked else None
                parts = []
                for d in range(D_STEP):
                    value = load(same, pl.ds(i * channels, channels), pl.ds(d * LANES, LANES))
                    parts.append(value.astype(jnp.bfloat16))
                halves.append(jnp.concatenate(parts, axis=0))
            projected = jnp.dot(w, jnp.concatenate(halves, axis=1), preferred_element_type=jnp.float32)
            for k in range(2):
                total[base + 2 * pair + k] += projected[:, k * LANES:(k + 1) * LANES]

    class Load:
        def __init__(self, first, paired, masked):
            self.first, self.paired, self.masked = first, paired, masked

        def __call__(self, same, piece, at):
            value = 0.0
            if self.masked:
                value = jnp.where(same, free_scr[piece, at], 0.0)
            if self.paired:
                value = outer_scr[piece, at] + value
            return value

    def multiply(ref, buffer, part, base):
        at = pl.ds(pl.multiple_of(base * channels, span), span)
        right = buffer[:, :, part].reshape(-1, WIDTH)
        return jnp.dot(left(ref, at), right, preferred_element_type=jnp.float32)

    groups = rows // group

    def compute(chunk, g):
        step = chunk // tiles
        turn = chunk % tiles
        first = col * tiles + tile_of(chunk)
        part = pl.ds(offset(chunk), WIDTH)
        mask_on = needed(FREE, chunk)
        total = acc.at[turn]
        w = weight[step]
        base = g * group

        @pl.when(g == 0)
        def _():
            gathered(chunk)

            @pl.when(step == 0)
            def _():
                total[...] = jnp.zeros_like(total)

        outer_scr[...] = multiply(left_pair, pair_buf, part, base)

        @pl.when(mask_on)
        def _():
            free_scr[...] = multiply(left_free, free_buf, part, base)
            project(w, Load(first, True, True), total, base)

        @pl.when(jnp.logical_not(mask_on))
        def _():
            project(w, Load(first, True, False), total, base)

    def help_compute(q, g):
        w = weight[q]
        first = (1 - col) * tiles + tile_of(q * tiles, 1 - col)
        part = pl.ds(offset(slot(q)), WIDTH)
        base = g * group

        @pl.when(g == 0)
        def _():
            from_sibling(FREE, slot(q))

            @pl.when(q == 0)
            def _():
                help_acc[...] = jnp.zeros_like(help_acc)

        free_scr[...] = multiply(left_free, free_buf, part, base)
        project(w, Load(first, False, True), help_acc, base)

        @pl.when((q == steps - 1) & (g == groups - 1))
        def _():
            @pl.loop(0, rows, unroll=4)
            def _(i):
                count = paired_total + depth_ref[i].astype(jnp.float32)
                help_out[i] = (help_acc[i] * (1.0 / count)).T.astype(help_out.dtype)

            result_copy().start()

    def scaled(turn, i):
        same = same_at(col * tiles + tile_of(turn), i)
        count = paired_total + jnp.where(same, depth_ref[i].astype(jnp.float32), 0.0)
        value = (acc[turn, i] * (1.0 / count)).T
        return value + bias[...] if final else value

    def store(turn, i, value):
        at = pl.ds(pl.multiple_of(tile_of(turn) * LANES, LANES), LANES)
        out_ref[i, at, :] = value.astype(out_ref.dtype)

    def finish(turn):
        def plain():
            @pl.loop(0, rows, unroll=4)
            def _(i):
                store(turn, i, scaled(turn, i))

        def hold():
            @pl.loop(0, rows, unroll=4)
            def _(i):
                acc[turn, i] = scaled(turn, i)

        if share and turn == 0:
            pl.when(asks)(hold)
            pl.when(jnp.logical_not(asks))(plain)
        else:
            plain()

    def combine():
        result_copy().wait_recv()

        @pl.loop(0, rows)
        def _(i):
            store(0, i, acc[0, i] + help_out[i].astype(jnp.float32))

    def work(turn, low, high):
        @pl.loop(low, high)
        def _(g):
            if share:
                helping(turn - HELP_LAG, lambda q: pl.when(helps)(lambda: help_compute(q, g)))
            within(turn - depth, chunks, lambda chunk: compute(chunk, g))

    start_at = min(depth, HELP_LAG)

    @pl.loop(0, chunks + depth)
    def _(turn):
        relay_line(turn)
        pl.when(turn > start_at)(lambda: work(turn, 0, groups // 2))
        relay_across(turn)

        @pl.when(turn == start_at)
        def _():
            for c in left_copies:
                c.wait()
            for c in local:
                c.wait()
            guarded(unhelping, own_free.wait)
            arrange(raw_pair, left_pair, False)
            arrange(raw_free, left_free, True)
            work(turn, 0, groups // 2)

        work(turn, groups // 2, groups)

        for done in range(tiles):
            pl.when(turn == chunks + depth - tiles + done)(functools.partial(finish, done))

    if share:
        pl.when(asks)(combine)

    @pl.loop(0, chunks)
    def _(chunk):
        drain(chunk)

    if share:
        pl.when(helps)(lambda: result_copy().wait_send())


def fused(right_pair, right_free, left_pair, left_free, weight, bias, lengths, depths, rows, paired_total, final):
    count, width = lax.axis_size("row"), lax.axis_size("col")
    layers = count // (Y_SIZE * CORES)
    channels = left_pair.shape[0] // rows
    out_channels = weight.shape[1]
    cols = right_pair.shape[1] // channels
    tiles, steps = cols // LANES, channels // D_STEP
    chunks = tiles * steps
    group = min(16, rows)
    share = width == 2 and tiles == 2 and layers == width * tiles and rows * count == layers * LANES
    smem = pl.BlockSpec(memory_space=pltpu.SMEM)
    vmem = pl.BlockSpec(memory_space=pltpu.VMEM)
    anywhere = pl.BlockSpec(memory_space=pl.ANY)
    helped = (rows, out_channels, LANES) if share else (8, 8, LANES)
    return pl.pallas_call(
        functools.partial(fused_kernel, layers, width, group, float(paired_total), final, share),
        out_shape=jax.ShapeDtypeStruct((rows, cols, out_channels), jnp.bfloat16 if final else jnp.float32),
        in_specs=[smem] * 2 + [anywhere] * 4 + [vmem] * 2,
        out_specs=vmem,
        scratch_shapes=[
            pltpu.SMEM((rows,), jnp.int32),
            pltpu.SMEM((rows,), jnp.int32),
            pltpu.SMEM((rows,), jnp.int32),
            pltpu.VMEM((steps, out_channels, D_STEP * channels), jnp.bfloat16),
            pltpu.VMEM(weight.shape, jnp.float32),
            pltpu.VMEM((left_pair.shape[0], LANES), jnp.float32),
            pltpu.VMEM((width,) + left_pair.shape, jnp.bfloat16),
            pltpu.VMEM((width,) + left_free.shape, jnp.bfloat16),
            pltpu.VMEM((count,) + right_pair.shape, jnp.bfloat16),
            pltpu.VMEM((count,) + right_free.shape, jnp.bfloat16),
            pltpu.VMEM((width,) + left_pair.shape, jnp.bfloat16),
            pltpu.VMEM((width,) + left_free.shape, jnp.bfloat16),
            pltpu.VMEM((group * channels, WIDTH), jnp.float32),
            pltpu.VMEM((group * channels, WIDTH), jnp.float32),
            pltpu.VMEM((tiles, rows, out_channels, LANES), jnp.float32),
            pltpu.VMEM(helped, jnp.float32),
            pltpu.VMEM((helped[0], helped[2], helped[1]), jnp.bfloat16),
            pltpu.VMEM((steps if share else 1, right_free.shape[0], WIDTH), jnp.bfloat16),
            pltpu.SemaphoreType.DMA((4, 2, chunks, count // CORES)),
            pltpu.SemaphoreType.DMA((2, chunks, count)),
            pltpu.SemaphoreType.DMA((2, width)),
            pltpu.SemaphoreType.DMA((2, width)),
            pltpu.SemaphoreType.DMA((4,)),
            pltpu.SemaphoreType.DMA((steps,)),
            pltpu.SemaphoreType.DMA((steps,)),
            pltpu.SemaphoreType.DMA((steps,)),
            pltpu.SemaphoreType.DMA((2,)),
        ],
        compiler_params=pltpu.CompilerParams(collective_id=0, has_side_effects=True, vmem_limit_bytes=60 << 20),
        name="gather_multiply",
    )(lengths, depths, right_pair, right_free, left_pair, left_free, weight, bias)


def flat_right(x):
    depth, channels, cols = x.shape
    return x.reshape(depth, channels, cols // LANES, LANES).transpose(0, 2, 1, 3).reshape(depth, -1)


def flat_left(x):
    depth, channels, rows = x.shape
    return x.transpose(1, 2, 0).reshape(channels * rows, depth)


def body(
    paired_left, paired_right, unpaired_left, unpaired_right,
    out_weight, out_bias, chain_lengths, unpaired_depths,
):
    rows = paired_left.shape[2]
    cols = paired_right.shape[2]
    seq = lax.axis_size("seq")
    bias = out_bias.reshape(1, -1)
    paired_total = paired_right.shape[0] * lax.axis_size("row") * seq
    out = fused(
        flat_right(paired_right), flat_right(unpaired_right), flat_left(paired_left), flat_left(unpaired_left),
        out_weight, bias, chain_lengths, unpaired_depths, rows, paired_total, seq == 1)
    if seq == 1:
        return out
    summed = lax.psum(out, "seq")
    share = cols // seq
    own = lax.dynamic_slice_in_dim(summed, lax.axis_index("seq") * share, share, 1)
    return (own + bias).astype(jnp.bfloat16)


def solution(mesh):
    return jax.shard_map(
        body,
        mesh=mesh,
        in_specs=(
            P(("groups", "seq", "col"), None, "row"),
            P(("groups", "seq", "row"), None, "col"),
            P(("groups", "seq", "col"), None, "row"),
            P(("groups", "seq", "row"), None, "col"),
            P(),
            P(),
            P("groups"),
            P("groups"),
        ),
        out_specs=P(("groups", "row"), ("col", "seq"), None),
        check_vma=False,
    )
```

```python
import functools

import jax
import jax.numpy as jnp
from jax import lax
from jax.experimental import pallas as pl
from jax.experimental.pallas import tpu as pltpu
from jax.sharding import PartitionSpec as P

LANES = 128
D_STEP = 8
WIDTH = D_STEP * LANES
LONGEST_CHAIN = 128
MESH = pl.DeviceIdType.MESH
Y_SIZE, CORES = 2, 2
AHEAD = 2
HELP_LAG = 3
PAIR_EARLY = 4
UP, DOWN, ACROSS, SIBLING = range(4)
PAIR, FREE = range(2)


def both(*terms):
    terms = [t for t in terms if t is not True]
    if any(t is False for t in terms):
        return False
    return functools.reduce(lambda a, b: a & b, terms) if terms else True


def guarded(condition, do):
    if condition is True:
        do()
    elif condition is not False:
        pl.when(condition)(do)


def fused_kernel(
    depth, width, group, paired_total, final, share,
    lengths_ref, depths_ref,
    pair_in, free_in, left_pair_in, left_free_in, plain_weight, bias,
    out_ref,
    start_ref, end_ref, depth_ref, weight, wide_weight, spread, raw_pair, raw_free,
    pair_buf, free_buf, left_pair, left_free, outer_scr, free_scr, acc, help_acc, help_out, via_buf,
    send_sem, recv_sem, left_send, left_recv, local_sem, via_send, via_recv, pass_send, help_sem,
):
    row, col = lax.axis_index("row"), lax.axis_index("col")
    core, y, z = row % CORES, (row // CORES) % Y_SIZE, row // (CORES * Y_SIZE)
    other = 1 - y
    rows, cols = out_ref.shape[0], out_ref.shape[1]
    channels = left_pair.shape[1] // rows
    tiles = cols // LANES
    steps = channels // D_STEP
    chunks = tiles * steps
    plane = rows * CORES * Y_SIZE
    span = group * channels

    def row_of(z_at, y_at, core_at):
        return (z_at * Y_SIZE + y_at) * CORES + core_at

    up, down = row_of(z + 1, y, core), row_of(z - 1, y, core)
    across, sibling = row_of(z, other, core), row_of(z, y, 1 - core)
    has_up, has_down = z < depth - 1, z > 0
    first_plane = jnp.where(col == 0, 0, depth - 1)
    last_plane = depth - 1 - first_plane
    asks = z == first_plane if share else False
    helps = z == last_plane if share else False
    distant = jnp.abs(z - last_plane) > 1 if share else False

    barrier = pltpu.get_barrier_semaphore()

    def greet(axis, at):
        pl.semaphore_signal(barrier, inc=1, device_id={axis: at}, device_id_type=MESH)

    pl.when(has_up)(lambda: greet("row", up))
    pl.when(has_down)(lambda: greet("row", down))
    greet("row", across)
    greet("row", sibling)
    for shift in range(1, width):
        greet("col", lax.rem(col + shift, width))
    met = jnp.where(has_up, 1, 0) + jnp.where(has_down, 1, 0) + 2 + width - 1
    if share:
        for hop in range(2, depth):
            far = jnp.where(last_plane == 0, hop, depth - 1 - hop)
            pl.when(helps)(functools.partial(greet, "row", row_of(far, y, core)))
        met = met + jnp.where(distant, 1, 0)
    pl.semaphore_wait(barrier, met)

    def tile_of(chunk, at_col=col):
        turn = chunk % tiles
        return jnp.where(at_col * 2 >= width, turn, tiles - 1 - turn)

    def offset(chunk, at_col=col):
        return pl.multiple_of((tile_of(chunk, at_col) * steps + chunk // tiles) * WIDTH, WIDTH)

    def reach(kind, chunk):
        if kind == PAIR:
            return 0, depth - 1
        first = (col * tiles + tile_of(chunk)) * LANES
        lowest = jnp.maximum(first - (LONGEST_CHAIN - 1), 0) // plane
        highest = jnp.minimum(first + LANES - 1 + (LONGEST_CHAIN - 1), depth * plane - 1) // plane
        if share:
            shared = chunk % tiles == 0
            lowest = jnp.where(shared & (col == 0), jnp.maximum(lowest, 1), lowest)
            highest = jnp.where(shared & (col > 0), jnp.minimum(highest, depth - 2), highest)
        return lowest, highest

    def needed(kind, chunk):
        if kind == PAIR:
            return True
        lowest, highest = reach(kind, chunk)
        return (z >= lowest) & (z <= highest)

    def early(kind, chunk):
        if kind == PAIR:
            return chunk % PAIR_EARLY == 0
        return chunk % tiles == 0 if share else False

    def late(kind, chunk):
        soon = early(kind, chunk)
        return True if soon is False else jnp.logical_not(soon)

    sources, buffers = (pair_in, free_in), (pair_buf, free_buf)

    def copy(kind, chunk, way, origin, target, own):
        part = pl.ds(offset(chunk), WIDTH)
        here = buffers[kind].at[origin, :, part]
        return pltpu.make_async_remote_copy(
            src_ref=sources[kind].at[:, part] if own else here, dst_ref=here,
            send_sem=send_sem.at[way, kind, chunk, origin // CORES], recv_sem=recv_sem.at[kind, chunk, origin],
            device_id={"row": target}, device_id_type=MESH)

    def move(c, started):
        c.start() if started else c.wait_send()

    def forward(kind, chunk, z_at, y_at, started):
        origin = row_of(z_at, y_at, core)
        line = y_at is y
        own = line and z_at is z
        lowest, highest = reach(kind, chunk)
        soon = early(kind, chunk)
        wanted = needed(kind, chunk)

        def go(way, target):
            move(copy(kind, chunk, way, origin, target, own), started)

        along = True if line else soon
        guarded(both(has_up, z_at <= z, z < highest, along), lambda: go(UP, up))
        guarded(both(has_down, z_at >= z, z > lowest, along), lambda: go(DOWN, down))
        if own:
            guarded(wanted if wanted is True or soon is False else wanted | soon, lambda: go(ACROSS, across))
        elif line:
            guarded(both(wanted, late(kind, chunk)), lambda: go(ACROSS, across))
        guarded(wanted, lambda: go(SIBLING, sibling))

    def arrive(kind, chunk, z_at, y_at, core_at):
        origin = row_of(z_at, y_at, core_at)
        copy(kind, chunk, SIBLING, origin, sibling, False).wait_recv()

    def hops(hop):
        if hop == 0:
            return ((z, True, None),)
        return ((z - hop, z >= hop, True), (z + hop, z + hop < depth, False))

    def arrivals(hop, y_at, chunk, visit):
        for kind in (PAIR, FREE):
            lowest, highest = reach(kind, chunk)
            for z_at, there, below in hops(hop):
                passes = True
                if kind == FREE and below is not None:
                    passes = (z <= highest) if below else (z >= lowest)
                if y_at is not y and kind == FREE:
                    soon = early(kind, chunk)
                    if soon is False:
                        passes = needed(kind, chunk)
                    else:
                        passes = (soon & passes) | (jnp.logical_not(soon) & needed(kind, chunk))
                guarded(both(there, passes), functools.partial(visit, kind, z_at, y_at))

    def onward(chunk, started):
        def visit(kind, z_at, y_at):
            if started:
                arrive(kind, chunk, z_at, y_at, core)
            forward(kind, chunk, z_at, y_at, started)
        return visit

    def slot(part):
        return part * tiles + 1

    def helping(turn, do):
        part = turn - turn // 3
        pl.when((turn >= 0) & (turn % 3 < 2) & (part < steps))(lambda: do(part))

    def via_copy(part, straight):
        target = free_buf.at[row, :, pl.ds(offset(slot(part), 1 - col), WIDTH)] if straight else via_buf.at[part]
        return pltpu.make_async_remote_copy(
            src_ref=free_in.at[:, pl.ds(offset(part * tiles), WIDTH)], dst_ref=target,
            send_sem=via_send.at[part], recv_sem=via_recv.at[part], device_id={"col": 1 - col}, device_id_type=MESH)

    def pass_copy(part):
        return pltpu.make_async_remote_copy(
            src_ref=via_buf.at[part], dst_ref=free_buf.at[row, :, pl.ds(offset(slot(part)), WIDTH)],
            send_sem=pass_send.at[part], recv_sem=recv_sem.at[FREE, slot(part), row],
            device_id={"row": row_of(last_plane, y, core)}, device_id_type=MESH)

    def via(part, started):
        pl.when(asks)(lambda: move(via_copy(part, True), started))
        pl.when(jnp.logical_not(asks))(lambda: move(via_copy(part, False), started))

    def help_spread(part, z_at, y_at, started):
        origin = row_of(z_at, y_at, core)
        if y_at is y:
            move(copy(FREE, slot(part), ACROSS, origin, across, False), started)
        move(copy(FREE, slot(part), SIBLING, origin, sibling, False), started)

    def help_first(part, started):
        if started:
            via_copy(part, False).wait_recv()

        @pl.when(jnp.logical_not(helps))
        def _():
            move(pass_copy(part), started)

        @pl.when(helps)
        def _():
            help_spread(part, z, y, started)

    def help_line(part, started):
        @pl.when(helps)
        def _():
            for hop in range(1, depth):
                z_at = jnp.where(last_plane == 0, hop, depth - 1 - hop)
                if started:
                    arrive(FREE, slot(part), z_at, y, core)
                help_spread(part, z_at, y, started)

    def help_last(part, started):
        @pl.when(helps)
        def _():
            for hop in range(depth):
                z_at = jnp.where(last_plane == 0, hop, depth - 1 - hop)
                if started:
                    arrive(FREE, slot(part), z_at, other, core)
                help_spread(part, z_at, other, started)

    def result_copy():
        return pltpu.make_async_remote_copy(
            src_ref=help_out, dst_ref=help_out, send_sem=help_sem.at[0], recv_sem=help_sem.at[1],
            device_id={"col": 1 - col}, device_id_type=MESH)

    def issue(chunk, started=True):
        for kind in (PAIR, FREE):
            forward(kind, chunk, z, y, started)

    def within(chunk, limit, do):
        pl.when((chunk >= 0) & (chunk < limit))(lambda: do(chunk))

    def relay_line(turn):
        for hop in range(1, depth):
            within(turn - (hop - 1), chunks, lambda chunk: arrivals(hop, y, chunk, onward(chunk, True)))
        if share:
            helping(turn, lambda part: help_first(part, True))
            helping(turn - 1, lambda part: help_line(part, True))

    def relay_across(turn):
        for hop in range(depth):
            within(turn - hop, chunks, lambda chunk: arrivals(hop, other, chunk, onward(chunk, True)))
        if share:
            helping(turn - 2, lambda part: help_last(part, True))
            helping(turn + AHEAD, lambda part: via(part, True))
        within(turn + AHEAD, chunks, issue)

    def drain(chunk):
        issue(chunk, False)
        for hop in range(depth):
            if hop:
                arrivals(hop, y, chunk, onward(chunk, False))
            arrivals(hop, other, chunk, onward(chunk, False))
        if share:
            @pl.when(chunk < steps)
            def _():
                via(chunk, False)
                help_first(chunk, False)
                help_line(chunk, False)
                help_last(chunk, False)

    def from_sibling(kind, chunk):
        for z_at in range(depth):
            for y_at in range(Y_SIZE):
                arrive(kind, chunk, z_at, y_at, 1 - core)

    def gathered(chunk):
        for kind in (PAIR, FREE):
            guarded(needed(kind, chunk), functools.partial(from_sibling, kind, chunk))

    for chunk in range(min(AHEAD, chunks)):
        if share:
            helping(jnp.int32(chunk), lambda part: via(part, True))
        issue(jnp.int32(chunk))

    left_copies = []
    local = [pltpu.make_async_copy(pair_in, pair_buf.at[row], local_sem.at[0])]
    own_free = pltpu.make_async_copy(free_in, free_buf.at[row], local_sem.at[1])
    unhelping = jnp.logical_not(helps) if share else True
    for n, (source, out) in enumerate(((left_pair_in, raw_pair), (left_free_in, raw_free))):
        mine = out.at[col]
        for shift in range(1, width):
            c = pltpu.make_async_remote_copy(
                src_ref=source, dst_ref=mine, send_sem=left_send.at[n, shift], recv_sem=left_recv.at[n, shift],
                device_id={"col": lax.rem(col + shift, width)}, device_id_type=MESH)
            c.start()
            left_copies.append(c)
        local.append(pltpu.make_async_copy(source, mine, local_sem.at[2 + n]))
    for c in local:
        c.start()
    guarded(unhelping, own_free.start)

    @pl.loop(0, rows)
    def _(i):
        place = row * rows + i
        end, start, stop, deep = jnp.int32(0), jnp.int32(0), jnp.int32(0), jnp.int32(0)
        for k in range(lengths_ref.shape[0]):
            begin, end = end, end + lengths_ref[k]
            mine = (place >= begin) & (place < end)
            start = jnp.where(mine, begin, start)
            stop = jnp.where(mine, end, stop)
            deep = jnp.where(mine, depths_ref[k], deep)
        start_ref[i], end_ref[i], depth_ref[i] = start, stop, deep

    wide_weight[...] = plain_weight[...].astype(jnp.float32)
    for step in range(steps):
        picked = [wide_weight[pl.ds(step * D_STEP + d, channels, stride=channels), :] for d in range(D_STEP)]
        weight[step] = jnp.concatenate(picked, axis=0).T.astype(jnp.bfloat16)

    def arrange(raw, arranged, masked):
        length = raw.shape[2]
        wide = min(length, LANES)
        for n in range(width):
            for low in range(0, length, wide):
                ids = lax.broadcasted_iota(jnp.int32, (1, LANES), 1) + n * length + low
                if masked:
                    ids = ids + lax.axis_index("seq") * (width * length)
                spread[:, :wide] = raw[n, :, low:low + wide].astype(jnp.float32)

                @pl.loop(0, rows, unroll=8)
                def _(i):
                    value = spread[pl.ds(i, channels, stride=rows), :]
                    if masked:
                        value = jnp.where(ids < depth_ref[i], value, 0.0)
                    at = pl.ds(pl.multiple_of(i * channels, channels), channels)
                    arranged[n, at, low:low + wide] = value[:, :wide].astype(jnp.bfloat16)

    def left(ref, at):
        return jnp.concatenate([ref[n, at, :] for n in range(width)], axis=1)

    def same_at(first, i):
        lanes = lax.broadcasted_iota(jnp.int32, (1, LANES), 1) + first * LANES
        return (lanes >= start_ref[i]) & (lanes < end_ref[i])

    def project(w, load, total, base):
        for pair in range(group // 2):
            halves = []
            for i in (2 * pair, 2 * pair + 1):
                same = same_at(load.first, base + i) if load.masked else None
                parts = []
                for d in range(D_STEP):
                    value = load(same, pl.ds(i * channels, channels), pl.ds(d * LANES, LANES))
                    parts.append(value.astype(jnp.bfloat16))
                halves.append(jnp.concatenate(parts, axis=0))
            projected = jnp.dot(w, jnp.concatenate(halves, axis=1), preferred_element_type=jnp.float32)
            for k in range(2):
                total[base + 2 * pair + k] += projected[:, k * LANES:(k + 1) * LANES]

    class Load:
        def __init__(self, first, paired, masked):
            self.first, self.paired, self.masked = first, paired, masked

        def __call__(self, same, piece, at):
            value = 0.0
            if self.masked:
                value = jnp.where(same, free_scr[piece, at], 0.0)
            if self.paired:
                value = outer_scr[piece, at] + value
            return value

    def multiply(ref, buffer, part, base):
        at = pl.ds(pl.multiple_of(base * channels, span), span)
        right = buffer[:, :, part].reshape(-1, WIDTH)
        return jnp.dot(left(ref, at), right, preferred_element_type=jnp.float32)

    groups = rows // group

    def compute(chunk, g):
        step = chunk // tiles
        turn = chunk % tiles
        first = col * tiles + tile_of(chunk)
        part = pl.ds(offset(chunk), WIDTH)
        mask_on = needed(FREE, chunk)
        total = acc.at[turn]
        w = weight[step]
        base = g * group

        @pl.when(g == 0)
        def _():
            gathered(chunk)

            @pl.when(step == 0)
            def _():
                total[...] = jnp.zeros_like(total)

        outer_scr[...] = multiply(left_pair, pair_buf, part, base)

        @pl.when(mask_on)
        def _():
            free_scr[...] = multiply(left_free, free_buf, part, base)
            project(w, Load(first, True, True), total, base)

        @pl.when(jnp.logical_not(mask_on))
        def _():
            project(w, Load(first, True, False), total, base)

    def help_compute(q, g):
        w = weight[q]
        first = (1 - col) * tiles + tile_of(q * tiles, 1 - col)
        part = pl.ds(offset(slot(q)), WIDTH)
        base = g * group

        @pl.when(g == 0)
        def _():
            from_sibling(FREE, slot(q))

            @pl.when(q == 0)
            def _():
                help_acc[...] = jnp.zeros_like(help_acc)

        free_scr[...] = multiply(left_free, free_buf, part, base)
        project(w, Load(first, False, True), help_acc, base)

        @pl.when((q == steps - 1) & (g == groups - 1))
        def _():
            @pl.loop(0, rows, unroll=8)
            def _(i):
                count = paired_total + depth_ref[i].astype(jnp.float32)
                help_out[i] = (help_acc[i] * (1.0 / count)).T.astype(help_out.dtype)

            result_copy().start()

    def scaled(turn, i):
        same = same_at(col * tiles + tile_of(turn), i)
        count = paired_total + jnp.where(same, depth_ref[i].astype(jnp.float32), 0.0)
        value = (acc[turn, i] * (1.0 / count)).T
        return value + bias[...] if final else value

    def store(turn, i, value):
        at = pl.ds(pl.multiple_of(tile_of(turn) * LANES, LANES), LANES)
        out_ref[i, at, :] = value.astype(out_ref.dtype)

    def finish(turn):
        def plain():
            @pl.loop(0, rows, unroll=8)
            def _(i):
                store(turn, i, scaled(turn, i))

        def hold():
            @pl.loop(0, rows, unroll=8)
            def _(i):
                acc[turn, i] = scaled(turn, i)

        if share and turn == 0:
            pl.when(asks)(hold)
            pl.when(jnp.logical_not(asks))(plain)
        else:
            plain()

    def combine():
        result_copy().wait_recv()

        @pl.loop(0, rows)
        def _(i):
            store(0, i, acc[0, i] + help_out[i].astype(jnp.float32))

    def work(turn, low, high):
        @pl.loop(low, high)
        def _(g):
            if share:
                helping(turn - HELP_LAG, lambda q: pl.when(helps)(lambda: help_compute(q, g)))
            within(turn - depth, chunks, lambda chunk: compute(chunk, g))

    start_at = min(depth, HELP_LAG)

    @pl.loop(0, chunks + depth)
    def _(turn):
        relay_line(turn)
        pl.when(turn > start_at)(lambda: work(turn, 0, groups // 2))
        relay_across(turn)

        @pl.when(turn == start_at)
        def _():
            for c in left_copies:
                c.wait()
            for c in local:
                c.wait()
            guarded(unhelping, own_free.wait)
            arrange(raw_pair, left_pair, False)
            arrange(raw_free, left_free, True)
            work(turn, 0, groups // 2)

        work(turn, groups // 2, groups)

        for done in range(tiles):
            pl.when(turn == chunks + depth - tiles + done)(functools.partial(finish, done))

    if share:
        pl.when(asks)(combine)

    @pl.loop(0, chunks)
    def _(chunk):
        drain(chunk)

    if share:
        pl.when(helps)(lambda: result_copy().wait_send())


def fused(right_pair, right_free, left_pair, left_free, weight, bias, lengths, depths, rows, paired_total, final):
    count, width = lax.axis_size("row"), lax.axis_size("col")
    layers = count // (Y_SIZE * CORES)
    channels = left_pair.shape[0] // rows
    out_channels = weight.shape[1]
    cols = right_pair.shape[1] // channels
    tiles, steps = cols // LANES, channels // D_STEP
    chunks = tiles * steps
    group = min(16, rows)
    share = width == 2 and tiles == 2 and layers == width * tiles and rows * count == layers * LANES
    smem = pl.BlockSpec(memory_space=pltpu.SMEM)
    vmem = pl.BlockSpec(memory_space=pltpu.VMEM)
    anywhere = pl.BlockSpec(memory_space=pl.ANY)
    helped = (rows, out_channels, LANES) if share else (8, 8, LANES)
    return pl.pallas_call(
        functools.partial(fused_kernel, layers, width, group, float(paired_total), final, share),
        out_shape=jax.ShapeDtypeStruct((rows, cols, out_channels), jnp.bfloat16 if final else jnp.float32),
        in_specs=[smem] * 2 + [anywhere] * 4 + [vmem] * 2,
        out_specs=vmem,
        scratch_shapes=[
            pltpu.SMEM((rows,), jnp.int32),
            pltpu.SMEM((rows,), jnp.int32),
            pltpu.SMEM((rows,), jnp.int32),
            pltpu.VMEM((steps, out_channels, D_STEP * channels), jnp.bfloat16),
            pltpu.VMEM(weight.shape, jnp.float32),
            pltpu.VMEM((left_pair.shape[0], LANES), jnp.float32),
            pltpu.VMEM((width,) + left_pair.shape, jnp.bfloat16),
            pltpu.VMEM((width,) + left_free.shape, jnp.bfloat16),
            pltpu.VMEM((count,) + right_pair.shape, jnp.bfloat16),
            pltpu.VMEM((count,) + right_free.shape, jnp.bfloat16),
            pltpu.VMEM((width,) + left_pair.shape, jnp.bfloat16),
            pltpu.VMEM((width,) + left_free.shape, jnp.bfloat16),
            pltpu.VMEM((group * channels, WIDTH), jnp.float32),
            pltpu.VMEM((group * channels, WIDTH), jnp.float32),
            pltpu.VMEM((tiles, rows, out_channels, LANES), jnp.float32),
            pltpu.VMEM(helped, jnp.float32),
            pltpu.VMEM((helped[0], helped[2], helped[1]), jnp.bfloat16),
            pltpu.VMEM((steps if share else 1, right_free.shape[0], WIDTH), jnp.bfloat16),
            pltpu.SemaphoreType.DMA((4, 2, chunks, count // CORES)),
            pltpu.SemaphoreType.DMA((2, chunks, count)),
            pltpu.SemaphoreType.DMA((2, width)),
            pltpu.SemaphoreType.DMA((2, width)),
            pltpu.SemaphoreType.DMA((4,)),
            pltpu.SemaphoreType.DMA((steps,)),
            pltpu.SemaphoreType.DMA((steps,)),
            pltpu.SemaphoreType.DMA((steps,)),
            pltpu.SemaphoreType.DMA((2,)),
        ],
        compiler_params=pltpu.CompilerParams(collective_id=0, has_side_effects=True, vmem_limit_bytes=60 << 20),
        name="gather_multiply",
    )(lengths, depths, right_pair, right_free, left_pair, left_free, weight, bias)


def flat_right(x):
    depth, channels, cols = x.shape
    return x.reshape(depth, channels, cols // LANES, LANES).transpose(0, 2, 1, 3).reshape(depth, -1)


def flat_left(x):
    depth, channels, rows = x.shape
    return x.transpose(1, 2, 0).reshape(channels * rows, depth)


def body(
    paired_left, paired_right, unpaired_left, unpaired_right,
    out_weight, out_bias, chain_lengths, unpaired_depths,
):
    rows = paired_left.shape[2]
    cols = paired_right.shape[2]
    seq = lax.axis_size("seq")
    bias = out_bias.reshape(1, -1)
    paired_total = paired_right.shape[0] * lax.axis_size("row") * seq
    out = fused(
        flat_right(paired_right), flat_right(unpaired_right), flat_left(paired_left), flat_left(unpaired_left),
        out_weight, bias, chain_lengths, unpaired_depths, rows, paired_total, seq == 1)
    if seq == 1:
        return out
    summed = lax.psum(out, "seq")
    share = cols // seq
    own = lax.dynamic_slice_in_dim(summed, lax.axis_index("seq") * share, share, 1)
    return (own + bias).astype(jnp.bfloat16)


def solution(mesh):
    return jax.shard_map(
        body,
        mesh=mesh,
        in_specs=(
            P(("groups", "seq", "col"), None, "row"),
            P(("groups", "seq", "row"), None, "col"),
            P(("groups", "seq", "col"), None, "row"),
            P(("groups", "seq", "row"), None, "col"),
            P(),
            P(),
            P("groups"),
            P("groups"),
        ),
        out_specs=P(("groups", "row"), ("col", "seq"), None),
        check_vma=False,
    )
```
